32 devices in a mesh: gx: 16 (over z, y, core), gy: 2 (over x).
Axes of the slice: x: 2, y: 2, z: 4, core: 2. Of those that a mesh axis runs over, the one named last changes fastest.
Arguments:
- right_side: float32 [16, 2, 512, 256], P('gx', 'gy'), may hold values from -8 to 8, as said below
- coords: float32 [16, 2, 2, 512], P('gx', 'gy'), may hold values from 0 to 1
- noise: float32 [16, 2, 512], P('gx', 'gy'), may hold values from 0.25 to 1
- intersect: int32 [16, 2, 128], P('gx', 'gy'), may hold values from 0 to 4607, as said below
Outputs:
- solution: float32 [16, 2, 512, 256], P('gx', 'gy')
- residual: float32 [16, 2, 512, 256], P('gx', 'gy')
The draws below stay inside these ranges and needn't reach their ends.
Inputs may be any that keep to these rules, and one draw needn't show every extreme that they name: `right_side`: right-hand sides of order one. `intersect`: each subdomain's list holds 128 distinct indices in increasing order; none names the subdomain itself (block number 4) or a subdomain beyond the first or last one along the second dimension.
All inputs are finite; a program needn't handle non-finite values.
Results may differ from the reference program's by a relative error of at most 0.0003.
Values sent between devices are 32-bit elements; how exact they have to be, the bound alone decides.
No kernel may reach another device: no remote copies, remote signals or barrier semaphores. Data moves between devices by JAX's collectives and lax.ppermute only.
A program may use at most 128 MiB of HBM per device.

```python
import math
import jax
import jax.numpy as jnp
from jax import lax

P_SIZE = 512
OV = 128
R = 256
ITERS = 3
CELLS_X = 16
CELLS_Y = 2


def draw_right_side(key, part):
    full_shape = (CELLS_X, CELLS_Y, P_SIZE, R)
    normal_vals = jax.random.normal(key, full_shape, jnp.float32)
    return jnp.clip(normal_vals, -6.0, 6.0)


def draw_intersect(key, part):
    slot_count = 9 * P_SIZE

    def per_cell(cell_id):
        cell_key = jax.random.fold_in(key, cell_id + 7)
        column_id = cell_id % CELLS_Y
        slot_ids = jnp.arange(slot_count, dtype=jnp.int32)
        block_col = slot_ids // P_SIZE % 3
        banned = (slot_ids // P_SIZE == 4) | (block_col == 0) & (column_id == 0) | (block_col == 2) & (column_id == CELLS_Y - 1)
        scores = jax.random.randint(cell_key, (slot_count,), 0, 131072, dtype=jnp.int32) * slot_count + slot_ids
        scores = jnp.where(banned, 1073741824 + slot_ids, scores)
        ranking = jnp.argsort(scores, stable=True)
        return jnp.sort(ranking[:OV]).astype(jnp.int32)
    chosen = jax.vmap(per_cell)(jnp.arange(CELLS_X * CELLS_Y, dtype=jnp.int32))
    return chosen.reshape(CELLS_X, CELLS_Y, OV)


def steps_of(stream_key, shape, shards, smallest, high):
    def one(position, parts):
        heights = jax.random.uniform(jax.random.fold_in(jax.random.fold_in(stream_key, 6), position), (parts,), jnp.float32, smallest / len(shards), high / len(shards))
        return jnp.repeat(jnp.exp(heights), shape[position] // parts).reshape((-1,) + (1,) * (len(shape) - position - 1))

    level = one(*shards[0])
    for cut in shards[1:]:
        level = level * one(*cut)
    return level


def setup_inputs(seed: int = 0) -> dict:
    keys = jax.random.split(jax.random.key(seed), 5)
    right_side = draw_right_side(jax.random.fold_in(keys[4], 71), 0)
    coords = jnp.clip(1.0 * jax.random.uniform(keys[1], (CELLS_X, CELLS_Y, 2, P_SIZE), jnp.float32) ** steps_of(keys[1], (CELLS_X, CELLS_Y, 2, P_SIZE), ((0, 16), (1, 2)), -0.2, 0.2), 0.0, 1.0)
    noise = jnp.clip(jnp.exp(math.log(1.0) - 1.3862944 * jax.random.uniform(keys[2], (CELLS_X, CELLS_Y, P_SIZE), jnp.float32) ** steps_of(keys[2], (CELLS_X, CELLS_Y, P_SIZE), ((0, 16), (1, 2)), -0.2, 0.2)), 0.25, 1.0)
    intersect = draw_intersect(jax.random.fold_in(keys[4], 71), 0)
    return {"right_side": right_side, "coords": coords, "noise": noise, "intersect": intersect}


RANGE_LEN = 0.25
ROOT_THREE = math.sqrt(3.0)
HIGH = lax.Precision.HIGHEST

def kernel_block(rows_pos, cols_pos):
    delta_x = rows_pos[0][:, None] - cols_pos[0][None, :]
    delta_y = rows_pos[1][:, None] - cols_pos[1][None, :]
    distance = jnp.sqrt(delta_x * delta_x + delta_y * delta_y)
    scaled = ROOT_THREE / RANGE_LEN * distance
    clipped = jnp.minimum(distance, 1.0)
    taper_val = jnp.square(jnp.square(1.0 - clipped)) * (4.0 * clipped + 1.0)
    return (1.0 + scaled) * jnp.exp(-scaled) * taper_val

def reference(right_side, coords, noise, intersect):
    cells_x, cells_y, points, rhs_count = right_side.shape
    intersect_len = intersect.shape[2]
    cell_count = cells_x * cells_y
    ext_len = points + intersect_len

    def neighbour(values, cell_row, cell_col, shift_x, shift_y):
        near_row = (cell_row + shift_x) % cells_x
        near_col = cell_col + shift_y
        inside = (near_col >= 0) & (near_col < cells_y)
        fetched = values[near_row, jnp.clip(near_col, 0, cells_y - 1)]
        return jnp.where(inside, fetched, jnp.zeros_like(fetched))

    def operate(vector):

        def per_cell(cell_id):
            cell_row = cell_id // cells_y
            cell_col = cell_id % cells_y
            own_pos = coords[cell_row, cell_col]
            accumulated = noise[cell_row, cell_col][:, None] * vector[cell_row, cell_col]
            for shift_x in (-1, 0, 1):
                for shift_y in (-1, 0, 1):
                    near_info = neighbour(coords, cell_row, cell_col, shift_x, shift_y)
                    near_pos = jnp.stack([near_info[0] + float(shift_x), near_info[1] + float(shift_y)])
                    near_vec = neighbour(vector, cell_row, cell_col, shift_x, shift_y)
                    accumulated = accumulated + jnp.dot(kernel_block(own_pos, near_pos).astype(jnp.float32), near_vec.astype(jnp.float32), precision=HIGH, preferred_element_type=jnp.float32)
            return accumulated
        result = lax.map(per_cell, jnp.arange(cell_count, dtype=jnp.int32))
        return result.reshape(cells_x, cells_y, points, rhs_count)

    def setup_cell(cell_id):
        cell_row = cell_id // cells_y
        cell_col = cell_id % cells_y
        intersect_ids = intersect[cell_row, cell_col]
        block_id = intersect_ids // points
        row_in = intersect_ids % points
        row_of = block_id // 3
        col_of = block_id % 3
        near_row = ((cell_row + row_of - 1) % cells_x).astype(jnp.int32)
        near_col = (cell_col + col_of - 1).astype(jnp.int32)
        pos_x = coords[near_row, near_col, 0, row_in]
        pos_y = coords[near_row, near_col, 1, row_in]
        ov_pos = jnp.stack([pos_x + (row_of - 1).astype(jnp.float32), pos_y + (col_of - 1).astype(jnp.float32)])
        ext_pos = jnp.concatenate([coords[cell_row, cell_col], ov_pos], axis=1)
        ext_noise = jnp.concatenate([noise[cell_row, cell_col], noise[near_row, near_col, row_in]])
        local_matrix = kernel_block(ext_pos, ext_pos) + jnp.diag(ext_noise)
        factor = jnp.linalg.cholesky(local_matrix)
        inv_factor = lax.linalg.triangular_solve(factor, jnp.eye(ext_len, dtype=jnp.float32), left_side=True, lower=True)
        inverse = jnp.dot(inv_factor.T.astype(jnp.float32), inv_factor.astype(jnp.float32), precision=HIGH, preferred_element_type=jnp.float32)
        global_ids = ((near_row * cells_y + near_col) * points + row_in).astype(jnp.int32)
        return (inverse, global_ids)
    inverses, global_ids = lax.map(setup_cell, jnp.arange(cell_count, dtype=jnp.int32))

    def precondition(residue):
        flat_res = residue.reshape(cell_count * points, rhs_count)
        extended = jnp.concatenate([residue.reshape(cell_count, points, rhs_count), flat_res[global_ids]], axis=1)
        solved = jnp.einsum('cij,cjr->cir', inverses, extended, precision=HIGH)
        result = solved[:, :points].reshape(cell_count * points, rhs_count)
        result = result.at[global_ids.reshape(-1)].add(solved[:, points:].reshape(-1, rhs_count))
        return result.reshape(cells_x, cells_y, points, rhs_count)

    def column_sum(first, second):
        return lax.optimization_barrier(jnp.sum(first * second, axis=(0, 1, 2)))
    solution = jnp.zeros_like(right_side)
    residual = right_side
    precond = precondition(residual)
    direction = precond
    inner_now = column_sum(residual, precond)
    for iteration in range(ITERS):
        image_vec = operate(direction)
        step_size = inner_now / column_sum(direction, image_vec)
        solution = solution + step_size * direction
        residual = residual - step_size * image_vec
        if iteration + 1 < ITERS:
            precond = precondition(residual)
            inner_next = column_sum(residual, precond)
            direction = precond + inner_next / inner_now * direction
            inner_now = inner_next
    return (solution, residual)
```

```python
import math

import jax
import jax.numpy as jnp
from jax import lax
from jax.experimental import pallas as pl
from jax.experimental.pallas import tpu as pltpu
from jax.sharding import PartitionSpec as P

ITERS = 3
BASIS_SHIFT = 1.75
NOISE_MIN = 0.25
NOISE_MAX = 1.0
RANGE_LEN = 0.25
ROOT_THREE = math.sqrt(3.0)
HIGH = lax.Precision.HIGHEST
LANES = 128
F32 = jnp.float32
BF16 = jnp.bfloat16


def params(*semantics, mib=12):
    return pltpu.CompilerParams(
        dimension_semantics=semantics or None, vmem_limit_bytes=mib * 2**20
    )


def kernel_of(delta_x, delta_y):
    square = delta_x * delta_x + delta_y * delta_y
    distance = square * lax.rsqrt(jnp.maximum(square, 1e-30))
    left = jnp.maximum(1.0 - distance, 0.0)
    quad = jnp.square(jnp.square(left))
    rate = ROOT_THREE / RANGE_LEN
    decay = jnp.exp2(distance * (-rate * math.log2(math.e)))
    return ((1.0 + rate * distance) * decay) * (quad * (5.0 - 4.0 * left))


def split(value):
    high = value.astype(BF16)
    return high, (value - high.astype(F32)).astype(BF16)


def mm(first, second, **kw):
    return jnp.dot(first, second, preferred_element_type=F32, **kw)


def mm3(first, second):
    first_h, first_l = split(first)
    second_h, second_l = split(second)
    return mm(first_h, second_h) + (mm(first_h, second_l) + mm(first_l, second_h))


def mm4(first, second):
    first_h, first_l = split(first)
    second_h, second_l = split(second)
    both = jnp.concatenate([first_h, first_l], axis=1)
    return mm(both, jnp.concatenate([second_h, second_h], axis=0)) + mm(
        both, jnp.concatenate([second_l, second_l], axis=0)
    )


def split3(value):
    high = value.astype(BF16)
    rest = value - high.astype(F32)
    middle = rest.astype(BF16)
    return high, middle, (rest - middle.astype(F32)).astype(BF16)


def mm6(first, second):
    fh, fm, fl = split3(first)
    sh, sm, sl = split3(second)
    both = jnp.concatenate([fh, fm], axis=1)
    ends = jnp.concatenate([fh, fl], axis=1)
    cat = lambda a, b: jnp.concatenate([a, b], axis=0)
    return mm(both, cat(sh, sh)) + (mm(both, cat(sm, sm)) + mm(ends, cat(sl, sh)))


def pair_of(value):
    high, low = split(value)
    return jnp.concatenate([high, low], axis=1)


def folded(product):
    half = product.shape[1] // 2
    return product[:, :half] + product[:, half:]


EARLY, LATE, UPDATE = mm3, mm6, mm6


def eye_mask(size):
    return lax.broadcasted_iota(jnp.int32, (size, size), 0) == lax.broadcasted_iota(
        jnp.int32, (size, size), 1
    )


def to_col(row):
    mask = eye_mask(LANES)
    parts = [
        jnp.sum(jnp.where(mask, row[:, k : k + LANES], 0.0), axis=1, keepdims=True)
        for k in range(0, row.shape[1], LANES)
    ]
    return parts[0] if len(parts) == 1 else jnp.concatenate(parts, axis=0)


def to_row(col):
    mask = eye_mask(LANES)
    parts = [
        jnp.sum(jnp.where(mask, col[k : k + LANES], 0.0), axis=0, keepdims=True)
        for k in range(0, col.shape[0], LANES)
    ]
    return parts[0] if len(parts) == 1 else jnp.concatenate(parts, axis=1)


def inverse_body(points, overlap, group, wx, wy, wn, picks, out_h, out_l, mat):
    extent = points + overlap
    block = LANES
    window = wx.shape[1]
    first_col = pl.program_id(0) * group
    for g in range(group):
        c = first_col + g
        own = pl.ds(pl.multiple_of(c * points, LANES), points)
        own_x, own_y, own_n = wx[:, own], wy[:, own], wn[:, own]
        pick = picks[c]
        pick_col = to_col(pick[0:1]).astype(jnp.int32)
        got = [jnp.zeros((overlap, 1), F32) for _ in range(3)]
        step = 512 if window % 512 == 0 else LANES
        for start in range(0, window, step):
            lane = lax.broadcasted_iota(jnp.int32, (overlap, step), 1) + start
            hit = lane == pick_col
            for m, ref in enumerate((wx, wy, wn)):
                got[m] = got[m] + jnp.sum(
                    jnp.where(hit, ref[:, start : start + step], 0.0), axis=1, keepdims=True
                )
        far_x, far_y, far_n = (to_row(v) for v in got)
        row_x = jnp.concatenate([own_x, far_x + pick[1:2]], axis=1)
        row_y = jnp.concatenate([own_y, far_y + pick[2:3]], axis=1)
        row_n = jnp.concatenate([own_n, far_n], axis=1)
        col_x, col_y = to_col(row_x), to_col(row_y)
        for start in range(0, extent, block):
            tile = kernel_of(
                col_x[start : start + block] - row_x, col_y[start : start + block] - row_y
            )
            sub = lax.broadcasted_iota(jnp.int32, (block, extent), 0) + start
            lane = lax.broadcasted_iota(jnp.int32, (block, extent), 1)
            mat[g, start : start + block, :] = tile + jnp.where(sub == lane, row_n, 0.0)

    identity = eye_mask(block).astype(F32)

    def block_inverses(schurs):
        low, high = NOISE_MIN, block + NOISE_MAX
        rho = (high - low) / (high + low)
        scale = 2.0 / (high + low)
        factor = 2.0 / (2.0 - rho * rho)
        found = [factor * scale * (2.0 * identity - scale * s) for s in schurs]
        rho = rho * rho / (2.0 - rho * rho)
        done = False
        while not done:
            done = rho < 1e-4
            factor = 1.0 if done else 2.0 / (2.0 - rho * rho)
            times = LATE if rho < 0.02 else EARLY
            images = [times(s, x) for s, x in zip(schurs, found)]
            found = [
                times(factor * x, 2.0 * identity - y) for x, y in zip(found, images)
            ]
            rho = rho * rho / (2.0 - rho * rho)
        return found

    def stage(k, carry):
        here = pl.ds(pl.multiple_of(k * block, block), block)
        pivots = block_inverses([mat[g, here, here] for g in range(group)])
        lane = lax.broadcasted_iota(jnp.int32, (block, extent), 1) - k * block
        sub = lax.broadcasted_iota(jnp.int32, (block, extent), 0)
        inside = (lane >= 0) & (lane < block)
        for g in range(group):
            row = jnp.where(inside, (lane == sub).astype(F32), mat[g, here, :])
            new_row = UPDATE(pivots[g], row)
            col = mat[g, :, here]
            mat[g, :, here] = jnp.zeros_like(col)
            for r in range(extent // block):
                rows = slice(r * block, (r + 1) * block)
                mat[g, rows, :] = mat[g, rows, :] - UPDATE(col[rows], new_row)
            mat[g, here, :] = new_row
        return carry

    lax.fori_loop(0, extent // block, stage, 0)
    for g in range(group):
        out_h[g], out_l[g] = split(mat[g])


def inverses(wx, wy, wn, picks, columns, points, overlap):
    extent = points + overlap
    group = 2 if columns % 2 == 0 else 1
    whole = lambda a: pl.BlockSpec(a.shape, lambda i: (0,) * a.ndim)
    out = pl.BlockSpec((group, extent, extent), lambda i: (i, 0, 0))
    return pl.pallas_call(
        lambda *refs: inverse_body(points, overlap, group, *refs),
        grid=(columns // group,),
        in_specs=[whole(wx), whole(wy), whole(wn), whole(picks)],
        out_specs=[out, out],
        out_shape=[jax.ShapeDtypeStruct((columns, extent, extent), BF16)] * 2,
        scratch_shapes=[pltpu.VMEM((group, extent, extent), F32)],
        compiler_params=params("arbitrary", mib=24),
        name="inverse",
    )(wx, wy, wn, picks)


def operator_block(own_x, own_y, far_x, far_y, points, rows, cols, is_self):
    tile = 128
    height = (rows[1] - rows[0]) * points
    width = (cols[1] - cols[0]) * points

    def body(ox, oy, fx, fy, out_h, out_l):
        first = pl.program_id(0) * tile
        c = rows[0] + first // points
        here = pl.ds(pl.multiple_of(rows[0] * points + first, LANES), tile)
        col_x, col_y = to_col(ox[:, here]), to_col(oy[:, here])
        for d in range(cols[0], cols[1]):
            there = slice(d * points, (d + 1) * points)
            value = kernel_of(
                col_x - fx[:, there], col_y - (fy[:, there] + (d - c).astype(F32))
            )
            if is_self:
                sub = lax.broadcasted_iota(jnp.int32, value.shape, 0) + first + rows[0] * points
                lane = lax.broadcasted_iota(jnp.int32, value.shape, 1) + d * points
                value = jnp.where(sub == lane, 0.0, value)
            put = slice((d - cols[0]) * points, (d - cols[0] + 1) * points)
            out_h[:, put], out_l[:, put] = split(value)

    whole = pl.BlockSpec(own_x.shape, lambda i: (0, 0))
    out = pl.BlockSpec((tile, width), lambda i: (i, 0))
    return pl.pallas_call(
        body,
        grid=(height // tile,),
        in_specs=[whole] * 4,
        out_specs=[out, out],
        out_shape=[jax.ShapeDtypeStruct((height, width), BF16)] * 2,
        compiler_params=params("arbitrary"),
        name="kern",
    )(own_x, own_y, far_x, far_y)


def multiply(blocks, vectors, base, tile=256):
    count = len(blocks)
    height, lanes = blocks[0][0].shape[0], vectors[0].shape[1]
    base = base if isinstance(base, tuple) else (base,)

    def body(*refs):
        mats, vecs = refs[: 2 * count], refs[2 * count : 3 * count]
        bases = refs[3 * count : 3 * count + len(base)]
        out = refs[3 * count + len(base)]
        packed = refs[3 * count + len(base) + 1 :]

        @pl.when(pl.program_id(0) == 0)
        def _():
            for vec, pack in zip(vecs, packed):
                pack[...] = pair_of(vec[...])

        total = bases[0][...]
        if len(bases) == 3:
            total = total * bases[1][...] - BASIS_SHIFT * bases[2][...]
        elif len(bases) == 2:
            total = total * bases[1][...]
        for k in range(count):
            for mat in mats[2 * k : 2 * k + 2]:
                total = total + folded(mm(mat[...], packed[k][...]))
        out[...] = total

    mats = [m for pair in blocks for m in pair]
    tiled = lambda width: pl.BlockSpec((tile, width), lambda i: (i, 0))
    return pl.pallas_call(
        body,
        grid=(height // tile,),
        in_specs=[tiled(m.shape[1]) for m in mats]
        + [pl.BlockSpec(v.shape, lambda i: (0, 0)) for v in vectors]
        + [tiled(lanes)] * len(base),
        out_specs=tiled(lanes),
        out_shape=jax.ShapeDtypeStruct((height, lanes), F32),
        scratch_shapes=[pltpu.VMEM((v.shape[0], 2 * lanes), BF16) for v in vectors],
        compiler_params=params("arbitrary"),
        name="multiply",
    )(*mats, *vectors, *base)


def gather_rows(selector, vector):
    def body(sel, vec, *outs):
        packed = pair_of(vec[...])
        for k, out in enumerate(outs):
            out[...] = folded(mm(sel[k], packed))

    count, height, _ = selector.shape
    shape = jax.ShapeDtypeStruct((height, vector.shape[1]), F32)
    return pl.pallas_call(
        body, out_shape=[shape] * count, compiler_params=params(), name="gather"
    )(selector, vector)


def solve(inv_h, inv_l, vector, borrowed, spread, points, overlap):
    columns = inv_h.shape[0]
    lanes = vector.shape[1]

    def body(ih, il, vec, b0, b1, b2, spr, own, back):
        for c in range(columns):
            rows = slice(c * points, (c + 1) * points)
            lent = slice(c * overlap, (c + 1) * overlap)
            ext = jnp.concatenate([vec[rows, :], b0[lent, :] + b1[lent, :] + b2[lent, :]], axis=0)
            packed = pair_of(ext)
            found = folded(mm(ih[c], packed)) + folded(mm(il[c], packed))
            own[rows, :] = found[:points]
            back[lent, :] = found[points:]
        own[...] = own[...] + folded(mm(spr[...], pair_of(back[...])))

    return pl.pallas_call(
        body,
        out_shape=[
            jax.ShapeDtypeStruct((columns * points, lanes), F32),
            jax.ShapeDtypeStruct((columns * overlap, lanes), F32),
        ],
        compiler_params=params(),
        name="solve",
    )(inv_h, inv_l, vector, *borrowed, spread)


def add_returned(spread_a, spread_b, part, back_a, back_b):
    def body(sa, sb, base, ba, bb, out):
        out[...] = (
            base[...]
            + folded(mm(sa[...], pair_of(ba[...])))
            + folded(mm(sb[...], pair_of(bb[...])))
        )

    return pl.pallas_call(
        body,
        out_shape=jax.ShapeDtypeStruct(part.shape, F32),
        compiler_params=params(),
        name="returned",
    )(spread_a, spread_b, part, back_a, back_b)


def gram(pairs, arrays):
    lanes = arrays[0].shape[1]

    def body(*refs):
        out = refs[-1]
        for row, (a, b) in enumerate(pairs):
            out[row : row + 1, :] = jnp.sum(refs[a][...] * refs[b][...], axis=0, keepdims=True)
        if len(pairs) < 8:
            out[len(pairs) :, :] = jnp.zeros((8 - len(pairs), lanes), F32)

    return pl.pallas_call(
        body,
        out_shape=jax.ShapeDtypeStruct((8, lanes), F32),
        compiler_params=params(),
        name="gram",
    )(*arrays)


def coefficients(inner):
    steps = ITERS
    shift = BASIS_SHIFT
    zero = jnp.zeros_like(inner[0][0])
    one = jnp.ones_like(zero)

    def image(d):
        out = [zero] * (steps + 1)
        for j in range(steps):
            if j + 1 < steps:
                out[j] = out[j] + shift * d[j]
            out[j + 1] = out[j + 1] + d[j]
        return out

    def product(a, b):
        total = zero
        for i in range(len(a)):
            if a[i] is zero:
                continue
            for j in range(len(b)):
                if b[j] is not zero:
                    total = total + a[i] * b[j] * inner[i][j]
        return total

    res = [one] + [zero] * steps
    direction = [one] + [zero] * (steps - 1)
    sol = [zero] * steps
    now = product(res[:steps], res[:steps])
    for k in range(steps):
        applied = image(direction)
        size = now / product(applied, direction)
        sol = [s + size * d for s, d in zip(sol, direction)]
        res = [r - size * a for r, a in zip(res, applied)]
        if k + 1 < steps:
            later = product(res[:steps], res[:steps])
            ratio = later / now
            direction = [r + ratio * d for r, d in zip(res[:steps], direction)]
            now = later
    return sol, res


def combine(totals, first, sols, ress, place, columns):
    count = len(sols)
    points, lanes = first.shape[0] // columns, first.shape[1]

    def body(place_ref, tot, b, *refs):
        vs, us = refs[:count], refs[count : 2 * count]
        out = refs[2 * count]
        sol, res = coefficients(unpack(lambda r: tot[r : r + 1, :]))
        x = sol[0] * vs[0][...]
        r = res[0] * b[...]
        for k in range(count):
            if k:
                x = x + sol[k] * vs[k][...]
            r = r + res[k + 1] * us[k][...]
        out[0, 0] = x
        out[0, 1] = r

    part = pl.BlockSpec((points, lanes), lambda d, p: (p[d], 0))
    return pl.pallas_call(
        body,
        grid_spec=pltpu.PrefetchScalarGridSpec(
            num_scalar_prefetch=1,
            grid=(columns,),
            in_specs=[pl.BlockSpec(totals.shape, lambda d, p: (0, 0)), part] + [part] * (2 * count),
            out_specs=pl.BlockSpec((1, 2, points, lanes), lambda d, p: (d, 0, 0, 0)),
        ),
        out_shape=jax.ShapeDtypeStruct((columns, 2, points, lanes), F32),
        compiler_params=params("arbitrary"),
        name="combine",
    )(place, totals, first, *sols, *ress)


def inner_rows():
    early = [(i, j) for i in range(ITERS) for j in range(i, ITERS)]
    late = [(ITERS, j) for j in range(ITERS)]
    return early, late


def unpack(value):
    early, late = inner_rows()
    table = [[None] * ITERS for _ in range(ITERS + 1)]
    for row, (i, j) in enumerate(early):
        table[i][j] = value(row)
        table[j][i] = value(row)
    for row, (i, j) in enumerate(late):
        table[i][j] = value(8 + row)
    return table


def shifted(value, axis, by):
    count = lax.axis_size(axis)
    return lax.ppermute(value, axis, [(i, (i + by) % count) for i in range(count)])


def passed_along(block, axis, distance):
    devices = range(lax.axis_size(axis))
    route = [(i - distance, i) for i in devices if i - distance in devices]
    return lax.ppermute(block, axis, route)


def plain_block(rows_pos, cols_pos):
    delta_x = rows_pos[0][:, None] - cols_pos[0][None, :]
    delta_y = rows_pos[1][:, None] - cols_pos[1][None, :]
    distance = jnp.sqrt(delta_x * delta_x + delta_y * delta_y)
    scaled = ROOT_THREE / RANGE_LEN * distance
    clipped = jnp.minimum(distance, 1.0)
    taper_val = jnp.square(jnp.square(1.0 - clipped)) * (4.0 * clipped + 1.0)
    return (1.0 + scaled) * jnp.exp(-scaled) * taper_val


def window_values(values):
    beside = {}
    for step_by in (1, -1):
        beside[step_by] = shifted(values, "gx", step_by)
    column = jnp.stack([beside[1], values, beside[-1]])
    across = {}
    for step_by in (1, -1):
        across[step_by] = passed_along(column, "gy", step_by)
    return [across[1], column, across[-1]]


def window_index(values):
    beside = {}
    for step_by in (1, -1):
        beside[step_by] = shifted(values, "gx", step_by)
    column = jnp.stack([beside[1], values, beside[-1]])
    across = {}
    for step_by in (1, -1):
        across[step_by] = passed_along(column, "gy", step_by)
    return [across[1], column, across[-1]]


def column_sum(first, second):
    return jnp.sum(first * second, axis=0)


def residual_dot(residue, precond):
    return lax.psum(column_sum(residue, precond), ("gx", "gy"))


def plain_shards(right_side, coords, noise, intersect):
    points = right_side.shape[2]
    rhs_count = right_side.shape[3]
    intersect_len = intersect.shape[2]
    ext_len = points + intersect_len
    own_pos = coords.reshape(2, points)
    own_noise = noise.reshape(points)
    point_info = jnp.concatenate([own_pos, own_noise[None, :]], axis=0)
    info_cols = window_values(point_info)
    positions = [
        [
            jnp.stack(
                [
                    info_cols[col_off][row_off, 0] + float(row_off - 1),
                    info_cols[col_off][row_off, 1] + float(col_off - 1),
                ]
            )
            for col_off in range(3)
        ]
        for row_off in range(3)
    ]
    intersect_ids = intersect.reshape(intersect_len)
    block_id = intersect_ids // points
    row_in = intersect_ids % points
    row_of = block_id // 3
    col_of = block_id % 3
    local_id = row_of * points + row_in
    picked_info = [
        jnp.take(
            jnp.transpose(info_cols[col_off], (1, 0, 2)).reshape(3, 3 * points), local_id, axis=1
        )
        for col_off in range(3)
    ]
    chosen = jnp.where(
        col_of[None, :] == 0,
        picked_info[0],
        jnp.where(col_of[None, :] == 1, picked_info[1], picked_info[2]),
    )
    ov_pos = jnp.stack(
        [chosen[0] + (row_of - 1).astype(jnp.float32), chosen[1] + (col_of - 1).astype(jnp.float32)]
    )
    ext_pos = jnp.concatenate([own_pos, ov_pos], axis=1)
    ext_noise = jnp.concatenate([own_noise, chosen[2]])
    local_matrix = plain_block(ext_pos, ext_pos) + jnp.diag(ext_noise)
    factor = jnp.linalg.cholesky(local_matrix)
    inv_factor = lax.linalg.triangular_solve(
        factor, jnp.eye(ext_len, dtype=jnp.float32), left_side=True, lower=True
    )
    inverse = jnp.dot(inv_factor.T, inv_factor, precision=HIGH, preferred_element_type=jnp.float32)
    near_ids = window_index(intersect_ids)
    point_iota = jnp.arange(points, dtype=jnp.int32)[:, None]
    row_base = (2 - jnp.arange(3, dtype=jnp.int32))[:, None] * 3
    selectors = []
    for col_off in range(3):
        own_rows = near_ids[col_off] - (row_base + (2 - col_off)) * points
        selectors.append((point_iota == own_rows.reshape(1, 3 * intersect_len)).astype(jnp.float32))

    def borrowed_rows(residue):
        requested = [
            lax.dot_general(
                selectors[col_off],
                residue,
                (((0,), (0,)), ((), ())),
                precision=HIGH,
                preferred_element_type=jnp.float32,
            ).reshape(3, intersect_len, rhs_count)
            for col_off in range(3)
        ]
        combined = jnp.stack([requested[col_off][1] for col_off in range(3)])
        for step_by, row_off in ((-1, 0), (1, 2)):
            outgoing = jnp.stack([requested[col_off][row_off] for col_off in range(3)])
            combined = combined + shifted(outgoing, "gx", step_by)
        gathered = combined[1]
        for step_by, col_off in ((-1, 0), (1, 2)):
            gathered = gathered + passed_along(combined[col_off], "gy", step_by)
        return gathered

    def precondition(residue):
        gathered = borrowed_rows(residue)
        extended = jnp.concatenate([residue, gathered], axis=0)
        solved = jnp.dot(inverse, extended, precision=HIGH, preferred_element_type=jnp.float32)
        returned = window_values(solved[points:])
        result = solved[:points]
        for col_off in range(3):
            result = result + jnp.dot(
                selectors[col_off],
                returned[col_off].reshape(3 * intersect_len, rhs_count),
                precision=HIGH,
                preferred_element_type=jnp.float32,
            )
        return result

    noise_col = own_noise[:, None]
    residual = right_side.reshape(points, rhs_count)
    solution = jnp.zeros_like(residual)
    precond = precondition(residual)
    direction = precond
    inner_now = residual_dot(residual, precond)
    for iteration in range(ITERS):
        columns = window_values(direction)
        accumulated = noise_col * direction
        for operate_row_off in range(3):
            for operate_col_off in range(3):
                accumulated = accumulated + jnp.dot(
                    plain_block(own_pos, positions[operate_row_off][operate_col_off]),
                    columns[operate_col_off][operate_row_off],
                    precision=HIGH,
                    preferred_element_type=jnp.float32,
                )
        step_size = inner_now / lax.psum(column_sum(direction, accumulated), ("gx", "gy"))
        solution = solution + step_size * direction
        residual = residual - step_size * accumulated
        if iteration + 1 < ITERS:
            precond = precondition(residual)
            inner_next = residual_dot(residual, precond)
            direction = precond + inner_next / inner_now * direction
            inner_now = inner_next
    return (solution.reshape(1, 1, points, rhs_count), residual.reshape(1, 1, points, rhs_count))


def ring_order(count):
    if count % 8:
        return list(range(count))
    depth = count // 4
    loop = [(z, 1) for z in range(depth)] + [(z, 0) for z in reversed(range(depth))]
    order = []
    for k in range(2 * depth):
        z, y = loop[(k - depth // 2) % (2 * depth)]
        order += [z * 4 + y * 2, z * 4 + y * 2 + 1]
    return order


def select(choices, index):
    out = choices[0]
    for k in range(1, len(choices)):
        out = jnp.where(index == k, choices[k], out)
    return out


def shards(right_side, coords, noise, intersect):
    points, rhs_count = right_side.shape[2:]
    overlap = intersect.shape[2]
    rows_x, columns = lax.axis_size("gx"), lax.axis_size("gy")
    lanes = rhs_count // columns
    both = ("gx", "gy")
    j = lax.axis_index("gy")
    order = ring_order(rows_x)
    parity = lax.axis_index("gx") % 2
    sign = (1 - 2 * parity).astype(F32)
    swap_a, swap_b = [], []
    for p in range(0, rows_x, 2):
        for swap, a, b in (
            (swap_a, order[p], order[p + 1]),
            (swap_b, order[p + 1], order[(p + 2) % rows_x]),
        ):
            swap += [(a, b), (b, a)]
    beside = lambda v: (lax.ppermute(v, "gx", swap_a), lax.ppermute(v, "gx", swap_b))

    def dealt(k):
        return [
            (i * columns + c, order[i] * columns + (c + k) % columns)
            for i in range(rows_x)
            for c in range(columns)
        ]

    def collected(k):
        return [
            (order[i] * columns + h, i * columns + (h + k) % columns)
            for i in range(rows_x)
            for h in range(columns)
        ]

    own = jnp.concatenate(
        [coords.reshape(2 * points), noise.reshape(points), intersect.reshape(overlap).astype(F32)]
    )
    got = [lax.ppermute(own, both, dealt(k)) for k in range(columns)]
    geometry = jnp.stack([select(got, (j - c) % columns) for c in range(columns)])
    rhs = right_side.reshape(points, rhs_count)
    pieces = [rhs[:, h * lanes : (h + 1) * lanes] for h in range(columns)]
    got = [
        lax.ppermute(select(pieces, (j + k) % columns), both, dealt(k)) for k in range(columns)
    ]
    start = jnp.concatenate([select(got, (j - c) % columns) for c in range(columns)], axis=0)
    geo_a, geo_b = beside(geometry)
    geos = [geometry, geo_a, geo_b]
    offsets = [jnp.zeros((), F32), sign, -sign]
    flat = lambda g, k: g[:, k * points : (k + 1) * points].reshape(1, columns * points)
    xs, ys, ns = ([flat(g, k) for g in geos] for k in range(3))
    wx, wy, wn = (jnp.concatenate(v, axis=1) for v in (xs, ys, ns))

    def decode(g):
        ids = g[:, 3 * points :].astype(jnp.int32)
        slot = ids // points
        return slot // 3 - 1, slot % 3 - 1, ids % points

    col_index = jnp.arange(columns, dtype=jnp.int32)[:, None]
    row_off, col_off, row_in = decode(geometry)
    side = jnp.where(row_off == 0, 0, jnp.where(row_off.astype(F32) == sign, 1, 2))
    local = side * (columns * points) + (col_index + col_off) * points + row_in
    picks = jnp.stack([v.astype(F32) for v in (local, row_off, col_off)], axis=1)
    wanted = []
    for g, off in zip(geos, offsets):
        row_off, col_off, row_in = decode(g)
        mine = row_off.astype(F32) == -off
        wanted.append(jnp.where(mine, (col_index + col_off) * points + row_in, -1).reshape(-1))
    wanted = jnp.stack(wanted)
    at = jnp.arange(columns * points, dtype=jnp.int32)
    selector = (wanted[:, :, None] == at).astype(BF16)
    spread = (wanted[:, None, :] == at[:, None]).astype(BF16)

    inv_h, inv_l = inverses(wx, wy, wn, picks, columns, points, overlap)
    whole = (0, columns)
    blocks = [
        operator_block(xs[0], ys[0], xs[t] + offsets[t], ys[t], points, whole, whole, t == 0)
        for t in range(3)
    ]
    scale = jnp.broadcast_to(
        1.0 + geometry[:, 2 * points : 3 * points].reshape(columns * points, 1),
        (columns * points, lanes),
    )

    def precondition(vector):
        lent, to_a, to_b = gather_rows(selector, vector)
        from_a = lax.ppermute(to_a, "gx", swap_a)
        from_b = lax.ppermute(to_b, "gx", swap_b)
        part, back = solve(
            inv_h, inv_l, vector, (lent, from_a, from_b), spread[0], points, overlap
        )
        back_a, back_b = beside(back)
        return add_returned(spread[1], spread[2], part, back_a, back_b)

    def operate(vector, before, last):
        near_a, near_b = beside(vector)
        base = (vector, scale) + (() if last else (before,))
        part = multiply(blocks[:2], [vector, near_a], base)
        return multiply([blocks[2]], [near_b], part)

    basis, images = [start], []
    for k in range(ITERS):
        images.append(precondition(basis[k]))
        basis.append(operate(images[k], basis[k], k + 1 == ITERS))

    early, late = inner_rows()
    first = gram([(i, ITERS + c) for i, c in early], basis[:ITERS] + images)
    second = gram([(0, 1 + c) for _, c in late], [basis[ITERS]] + images)
    totals = jnp.concatenate([first, second], axis=0)

    def exchanged(value, distance):
        return lax.ppermute(value, "gx", [(g, g ^ distance) for g in range(rows_x)])

    bits = [1 << b for b in range(rows_x.bit_length() - 1)]
    for step in [bits[:1], bits[1:2]] + [bits[k : k + 2] for k in range(2, len(bits), 2)]:
        routes = step if len(step) < 2 else [step[0], step[1], step[0] ^ step[1]]
        totals = totals + sum(exchanged(totals, r) for r in routes)

    turn = (j + jnp.arange(columns, dtype=jnp.int32)) % columns
    ready = combine(totals, start, images, basis[1:], turn, columns)
    sent = [lax.ppermute(ready[k], both, collected(k)) for k in range(columns)]
    outs = []
    for part in range(2):
        pieces = [select([s[part] for s in sent], (j - h) % columns) for h in range(columns)]
        outs.append(jnp.concatenate(pieces, axis=1).reshape(1, 1, points, rhs_count))
    return tuple(outs)


def solution(mesh):
    placed = (
        P("gx", "gy", None, None),
        P("gx", "gy", None, None),
        P("gx", "gy", None),
        P("gx", "gy", None),
    )
    rows_x, columns = mesh.shape["gx"], mesh.shape["gy"]
    paired = columns == 2 and rows_x >= 4 and rows_x & (rows_x - 1) == 0
    return jax.shard_map(
        shards if paired else plain_shards,
        mesh=mesh,
        in_specs=placed,
        out_specs=(P("gx", "gy", None, None), P("gx", "gy", None, None)),
        check_vma=False,
    )
```
